32 devices in a mesh: dp: 4 (over z), tensor: 8 (over y, x, core).
Axes of the slice: x: 2, y: 2, z: 4, core: 2. Of those that a mesh axis runs over, the one named last changes fastest.
Arguments:
- activations: bfloat16 [16384, 4096], P(('dp', 'tensor')), may hold values from -6 to 6
- cotangent: bfloat16 [16384, 11008], P('dp', 'tensor'), may hold values from -0.016357422 to 0.016357422
- projection: bfloat16 [4096, 512], replicated, may hold values from -0.25 to 0.25
- first_moment: float32 [512, 11008], P('dp', 'tensor'), may hold values from -0.6 to 0.6
- second_moment: float32 [512, 11008], P('dp', 'tensor'), may hold values from 0.01 to 1
- step_count: int32 [1], replicated, may hold values from 1 to 39
Outputs:
- update: bfloat16 [4096, 11008], P('dp', 'tensor')
- new_first: float32 [512, 11008], P('dp', 'tensor')
- new_second: float32 [512, 11008], P('dp', 'tensor')
The draws below stay inside these ranges and needn't reach their ends.
All inputs are finite; a program needn't handle non-finite values.
Results may differ from the reference program's by a relative error of at most 0.0055.
Values may be sent and summed in bfloat16 or wider, within the bound.
No kernel may reach another device: no remote copies, remote signals or barrier semaphores. Data moves between devices by JAX's collectives and lax.ppermute only.
A program may use at most 128 MiB of HBM per device.

```python
import math
import jax
import jax.numpy as jnp
from jax import lax

D = 4096
F = 11008
R = 512
TOKENS = 16384


def block_scale(rng, extent, pieces, least, top_value):
    loudness = 1.0
    for axis_at, blocks in pieces:
        heights = jax.random.uniform(jax.random.fold_in(jax.random.fold_in(rng, 6), axis_at), (blocks,), jnp.float32, least / len(pieces), top_value / len(pieces))
        loudness = loudness * jnp.repeat(jnp.exp(heights), extent[axis_at] // blocks).reshape((-1,) + (1,) * (len(extent) - 1 - axis_at))
    return loudness


def normal_values(stream_key, shape, width, reach, cuts=(), dtype=jnp.bfloat16):
    array = width * jax.random.normal(stream_key, shape, jnp.float32)
    if cuts:
        array = array * block_scale(stream_key, shape, cuts, -0.22, 0.18)
    return jnp.clip(array, -reach, reach).astype(dtype)


def setup_inputs(seed: int = 0) -> dict:
    seeds = jax.random.split(jax.random.key(seed), 7)
    return {
        "activations": normal_values(seeds[0], (TOKENS, D), 1.0, 6.0, ((0, 32),)),
        "cotangent": normal_values(seeds[1], (TOKENS, F), (0.35 / (TOKENS) ** 0.5), 0.016357422, ((0, 4), (1, 8))),
        "projection": normal_values(seeds[2], (D, R), R ** -0.5, 0.25),
        "first_moment": normal_values(seeds[3], (R, F), 0.1, 0.6, ((0, 4), (1, 8)), jnp.float32),
        "second_moment": jnp.clip(jnp.exp(math.log(1.0) - 4.6051702 * jax.random.uniform(seeds[4], (R, F), jnp.float32) ** block_scale(seeds[4], (R, F), ((0, 4), (1, 8)), -0.2, 0.2)), 0.01, 1.0),
        "step_count": jax.random.randint(seeds[5], (1,), 1, 40).astype(jnp.int32),
    }


def reference(activations, cotangent, projection, first_moment, second_moment, step_count):
    projected = jnp.dot(activations, projection, preferred_element_type=jnp.float32).astype(jnp.bfloat16)
    grad = lax.dot_general(projected, cotangent, (((0,), (0,)), ((), ())), preferred_element_type=jnp.float32)
    t_value = step_count[0].astype(jnp.float32)
    new_first = 0.9 * first_moment + 0.1 * grad
    new_second = 0.999 * second_moment + 0.001 * grad * grad
    first_hat = new_first / (1.0 - jnp.power(jnp.float32(0.9), t_value))
    second_hat = new_second / (1.0 - jnp.power(jnp.float32(0.999), t_value))
    normalized = (first_hat / (jnp.sqrt(second_hat) + 1e-08)).astype(jnp.bfloat16)
    update = jnp.dot(projection, normalized, preferred_element_type=jnp.float32).astype(jnp.bfloat16)
    return (update, new_first, new_second)
```

```python
import jax
import jax.numpy as jnp
import numpy as np
from jax import lax
from jax.experimental import pallas as pl
from jax.experimental.pallas import tpu as pltpu
from jax.sharding import PartitionSpec as P


F32 = jnp.float32
BF16 = jnp.bfloat16
LANES = 128


def adam(grad, first_moment, second_moment, step_count):
    t_value = step_count[0].astype(F32)
    new_first = 0.9 * first_moment + 0.1 * grad
    new_second = 0.999 * second_moment + 0.001 * grad * grad
    first_hat = new_first / (1.0 - jnp.power(F32(0.9), t_value))
    second_hat = new_second / (1.0 - jnp.power(F32(0.999), t_value))
    normalized = (first_hat / (jnp.sqrt(second_hat) + 1e-08)).astype(BF16)
    return new_first, new_second, normalized


def plain(activations, cotangent, projection, first_moment, second_moment, step_count):
    projected = jnp.dot(activations, projection, preferred_element_type=F32).astype(BF16)
    partial_grad = lax.dot_general(
        lax.all_gather(projected, "tensor", axis=0, tiled=True),
        cotangent,
        (((0,), (0,)), ((), ())),
        preferred_element_type=F32,
    )
    grad = lax.psum_scatter(partial_grad, "dp", scatter_dimension=0, tiled=True)
    new_first, new_second, normalized = adam(grad, first_moment, second_moment, step_count)
    whole_steps = lax.all_gather(normalized, "dp", axis=0, tiled=True)
    out_rows = projection.shape[0] // lax.axis_size("dp")
    local_projection = lax.dynamic_slice_in_dim(
        projection, lax.axis_index("dp") * out_rows, out_rows, 0
    )
    update = jnp.dot(local_projection, whole_steps, preferred_element_type=F32).astype(BF16)
    return update, new_first, new_second


def tile_of(extent, most=512):
    return max(d for d in range(8, most + 1, 8) if extent % d == 0)


def swap(x, axis, mask):
    return lax.ppermute(x, axis, [(i, i ^ mask) for i in range(lax.axis_size(axis))])


def swap_by_core(x, masks):
    return lax.ppermute(x, "tensor", [(i, i ^ masks[i % 2]) for i in range(lax.axis_size("tensor"))])


def project(table, activations, projection, first):
    rows, width = activations.shape
    depth = width // 4

    def kernel(tab, a, w0, w1, out, acc):
        k = pl.program_id(0)
        w = jnp.concatenate([w0[...], w1[...]], axis=1)
        part = jnp.dot(a[...], w, preferred_element_type=F32)

        @pl.when(k == 0)
        def _():
            acc[...] = part

        @pl.when(k > 0)
        def _():
            acc[...] += part

        @pl.when(k == pl.num_programs(0) - 1)
        def _():
            out[...] = acc[...].astype(BF16)

    return pl.pallas_call(
        kernel,
        grid_spec=pltpu.PrefetchScalarGridSpec(
            num_scalar_prefetch=1,
            grid=(4,),
            in_specs=[
                pl.BlockSpec((rows, depth), lambda k, tab: (0, k)),
                pl.BlockSpec((depth, LANES), lambda k, tab: (k, tab[first])),
                pl.BlockSpec((depth, LANES), lambda k, tab: (k, tab[first + 1])),
            ],
            out_specs=pl.BlockSpec((rows, 2 * LANES), lambda k, tab: (0, 0)),
            scratch_shapes=[pltpu.VMEM((rows, 2 * LANES), F32)],
        ),
        out_shape=jax.ShapeDtypeStruct((rows, 2 * LANES), BF16),
        cost_estimate=pl.CostEstimate(
            flops=4 * rows * width * LANES,
            bytes_accessed=2 * width * (rows + 2 * LANES),
            transcendentals=0,
        ),
        compiler_params=pltpu.CompilerParams(vmem_limit_bytes=32 << 20),
        name="project",
    )(table, activations, projection, projection)


def token_sum(table, cot_t, blocks, first, total, halves):
    f_local = cot_t.shape[0]
    rows, cols = blocks[0].shape
    tile = tile_of(f_local // 2)
    per_half = f_local // 2 // tile
    n = len(blocks)
    has_total = total is not None

    def kernel(tab, *refs):
        cots, projected, rest = refs[:n], refs[n : 2 * n], refs[2 * n :]
        i = pl.program_id(0)
        acc = jnp.dot(cots[0][...], projected[0][...], preferred_element_type=F32)
        for c, p in zip(cots[1:], projected[1:]):
            acc += jnp.dot(c[...], p[...], preferred_element_type=F32)
        if has_total:
            acc += rest[0][...]
            rest = rest[1:]
        if halves:

            @pl.when(i < per_half)
            def _():
                rest[0][...] = acc.astype(BF16)

            @pl.when(i >= per_half)
            def _():
                rest[1][...] = acc.astype(BF16)
        else:
            rest[0][...] = acc

    cot_specs = [
        pl.BlockSpec((tile, rows), lambda i, tab, j=j: (i, tab[4 + first + j])) for j in range(n)
    ]
    block_specs = [pl.BlockSpec((rows, cols), lambda i, tab: (0, 0)) for _ in range(n)]
    whole = pl.BlockSpec((tile, cols), lambda i, tab: (i, 0))
    if halves:
        out_specs = [
            pl.BlockSpec((tile, cols), lambda i, tab: (jnp.minimum(i, per_half - 1), 0)),
            pl.BlockSpec((tile, cols), lambda i, tab: (jnp.maximum(i - per_half, 0), 0)),
        ]
        out_shape = [jax.ShapeDtypeStruct((f_local // 2, cols), BF16)] * 2
    else:
        out_specs = whole
        out_shape = jax.ShapeDtypeStruct((f_local, cols), F32)
    return pl.pallas_call(
        kernel,
        grid_spec=pltpu.PrefetchScalarGridSpec(
            num_scalar_prefetch=1,
            grid=(2 * per_half,),
            in_specs=cot_specs + block_specs + [whole] * has_total,
            out_specs=out_specs,
        ),
        out_shape=out_shape,
        cost_estimate=pl.CostEstimate(
            flops=2 * n * rows * cols * f_local,
            bytes_accessed=2 * n * rows * (f_local + cols) + 4 * f_local * cols,
            transcendentals=0,
        ),
        compiler_params=pltpu.CompilerParams(vmem_limit_bytes=32 << 20),
        name="token_sum",
    )(table, *[cot_t] * n, *blocks, *([total] if has_total else []))


def apply_steps(table, steps, projection, f_local, half, out):
    rows = projection.shape[0] // lax.axis_size("dp")
    f_half = f_local // 2
    tile = tile_of(f_half)
    per_half = f_half // tile
    order = (2, 3, 0, 1)

    def kernel(tab, *refs):
        x = jnp.concatenate([r[...] for r in refs[:4]], axis=1)
        w = jnp.concatenate([r[...] for r in refs[4:8]], axis=1)
        refs[-1][...] = lax.dot_general(
            x, w, (((1,), (1,)), ((), ())), preferred_element_type=F32
        ).astype(BF16)

    in_specs = [pl.BlockSpec((tile, LANES), lambda i, tab: (i, 0)) for _ in range(4)]
    in_specs += [
        pl.BlockSpec((rows, LANES), lambda i, tab, j=j: (tab[2], tab[j])) for j in order
    ]
    extra = []
    if out is not None:
        in_specs.append(pl.BlockSpec(memory_space=pl.ANY))
        extra = [out]
    return pl.pallas_call(
        kernel,
        grid_spec=pltpu.PrefetchScalarGridSpec(
            num_scalar_prefetch=1,
            grid=(per_half,),
            in_specs=in_specs,
            out_specs=pl.BlockSpec((tile, rows), lambda i, tab: (i + half * per_half, 0)),
        ),
        out_shape=jax.ShapeDtypeStruct((f_local, rows), BF16),
        input_output_aliases={9: 0} if extra else {},
        cost_estimate=pl.CostEstimate(
            flops=8 * f_half * LANES * rows,
            bytes_accessed=2 * f_half * (rows + 4 * LANES) + 8 * rows * LANES,
            transcendentals=0,
        ),
        compiler_params=pltpu.CompilerParams(vmem_limit_bytes=32 << 20),
        name="apply_steps",
    )(table, *steps, *[projection] * 4, *extra)


def gather_blocks(own):
    first, second = (2, 4), (4, 2)
    far = swap_by_core(own, first)
    partner = swap(own, "tensor", 1)
    far_partner = swap_by_core(partner, first)
    corner = swap_by_core(far, second)
    other_far = swap(far, "tensor", 1)
    other_far_partner = swap(far_partner, "tensor", 1)
    other_corner = swap(corner, "tensor", 1)
    return [own, partner, far, far_partner, other_far, other_far_partner, corner, other_corner]


EVEN = (1, 3, 0, 2, 0, 1, 2, 3, 5, 4, 6, 7)
ODD = (1, 3, 0, 2, 0, 1, 4, 5, 3, 2, 6, 7)


def stepped(activations, cotangent, projection, first_moment, second_moment, step_count):
    tensor, replica = lax.axis_index("tensor"), lax.axis_index("dp")
    masks = jnp.where(tensor % 2 == 0, np.array(EVEN, np.int32), np.array(ODD, np.int32))
    table = jnp.where(np.arange(len(EVEN)) < 4, replica, tensor).astype(jnp.int32) ^ masks
    cot_t = cotangent.T
    f_local = cot_t.shape[0]
    f_half = f_local // 2

    away = gather_blocks(project(table, activations, projection, 0))
    home = gather_blocks(project(table, activations, projection, 2))
    sums = []
    for blocks, halves in ((away, True), (home, False)):
        total = token_sum(table, cot_t, blocks[:6], 0, None, False)
        sums.append(token_sum(table, cot_t, blocks[6:], 6, total, halves))
    to_send, kept = sums

    update, firsts, seconds = None, [], []
    for half in range(2):
        part = slice(half * f_half, (half + 1) * f_half)
        met = swap(to_send[half], "dp", 1)
        across = swap((kept[part, LANES:] + met[:, LANES:]).astype(BF16), "dp", 2)
        grad = kept[part, :LANES] + met[:, :LANES] + across
        new_first, new_second, normalized = adam(
            grad, first_moment.T[part], second_moment.T[part], step_count
        )
        firsts.append(new_first)
        seconds.append(new_second)
        step_2 = swap(normalized, "dp", 2)
        step_1 = swap(normalized, "dp", 1)
        step_3 = swap(step_2, "dp", 1)
        update = apply_steps(
            table, [normalized, step_2, step_1, step_3], projection, f_local, half, update
        )
    return update.T, jnp.concatenate(firsts).T, jnp.concatenate(seconds).T


def solution(mesh):
    in_specs = (
        P(("dp", "tensor"), None),
        P("dp", "tensor"),
        P(),
        P("dp", "tensor"),
        P("dp", "tensor"),
        P(),
    )
    out_specs = (P("dp", "tensor"), P("dp", "tensor"), P("dp", "tensor"))
    exchanges = mesh.shape["dp"] == 4 and mesh.shape["tensor"] == 8

    def per_device(activations, cotangent, projection, first_moment, second_moment, step_count):
        fits = (
            exchanges
            and first_moment.shape[0] == LANES
            and cotangent.shape[1] % 16 == 0
            and activations.shape[0] % LANES == 0
        )
        return (stepped if fits else plain)(
            activations, cotangent, projection, first_moment, second_moment, step_count
        )

    return jax.shard_map(
        per_device, mesh=mesh, in_specs=in_specs, out_specs=out_specs, check_vma=False
    )
```

```python
import jax
import jax.numpy as jnp
import numpy as np
from jax import lax
from jax.experimental import pallas as pl
from jax.experimental.pallas import tpu as pltpu
from jax.sharding import PartitionSpec as P


F32 = jnp.float32
BF16 = jnp.bfloat16
PROJECT_VMEM = 51 << 20
TOKEN_VMEM = 16 << 20
APPLY_VMEM = 12 << 20
SMALL_VMEM = 4 << 20
LOAD_VMEM = 47 << 20
TOKEN_TILE = 344
LANES = 128


def adam(grad, first_moment, second_moment, step_count):
    t_value = step_count[0].astype(F32)
    new_first = 0.9 * first_moment + 0.1 * grad
    new_second = 0.999 * second_moment + 0.001 * grad * grad
    first_hat = new_first / (1.0 - jnp.power(F32(0.9), t_value))
    second_hat = new_second / (1.0 - jnp.power(F32(0.999), t_value))
    normalized = (first_hat / (jnp.sqrt(second_hat) + 1e-08)).astype(BF16)
    return new_first, new_second, normalized


def plain(activations, cotangent, projection, first_moment, second_moment, step_count):
    projected = jnp.dot(activations, projection, preferred_element_type=F32).astype(BF16)
    partial_grad = lax.dot_general(
        lax.all_gather(projected, "tensor", axis=0, tiled=True),
        cotangent,
        (((0,), (0,)), ((), ())),
        preferred_element_type=F32,
    )
    grad = lax.psum_scatter(partial_grad, "dp", scatter_dimension=0, tiled=True)
    new_first, new_second, normalized = adam(grad, first_moment, second_moment, step_count)
    whole_steps = lax.all_gather(normalized, "dp", axis=0, tiled=True)
    out_rows = projection.shape[0] // lax.axis_size("dp")
    local_projection = lax.dynamic_slice_in_dim(
        projection, lax.axis_index("dp") * out_rows, out_rows, 0
    )
    update = jnp.dot(local_projection, whole_steps, preferred_element_type=F32).astype(BF16)
    return update, new_first, new_second


def tile_of(extent, most=512):
    return max(d for d in range(8, most + 1, 8) if extent % d == 0)


def swap(x, axis, mask):
    return lax.ppermute(x, axis, [(i, i ^ mask) for i in range(lax.axis_size(axis))])


def swap_by_core(x, masks):
    return lax.ppermute(
        x, "tensor", [(i, i ^ masks[i % 2]) for i in range(lax.axis_size("tensor"))]
    )


def row_blocks():
    replica = lax.axis_index("dp")
    return [replica ^ mask for mask in (1, 3, 0, 2)]


def lanes_of(index, size):
    return pl.ds(pl.multiple_of(index * size, size), size)


IN_VMEM = pl.BlockSpec(memory_space=pltpu.VMEM)
ANYWHERE = pl.BlockSpec(memory_space=pl.ANY)


def project(activations, projection):
    rows, width = activations.shape
    rank = projection.shape[1]
    steps = 8
    depth = width // steps

    def kernel(a_hbm, w_hbm, first, second, a_buf, w_buf, acc, sems):
        copies = []
        for k in range(steps):
            part = pl.ds(k * depth, depth)
            a_copy = pltpu.make_async_copy(a_hbm.at[:, part], a_buf.at[k], sems.at[2 * k])
            w_copy = pltpu.make_async_copy(w_hbm.at[part, :], w_buf.at[k], sems.at[2 * k + 1])
            a_copy.start()
            w_copy.start()
            copies.append((a_copy, w_copy))
        total = None
        for k, (a_copy, w_copy) in enumerate(copies):
            a_copy.wait()
            w_copy.wait()
            part = jnp.dot(a_buf[k], w_buf[k], preferred_element_type=F32)
            total = part if total is None else total + part
        acc[...] = total
        for j, block in enumerate(row_blocks()):
            out = (first, second)[j // 2]
            out[:, (j % 2) * LANES : (j % 2 + 1) * LANES] = acc[:, lanes_of(block, LANES)].astype(BF16)

    return pl.pallas_call(
        kernel,
        in_specs=[ANYWHERE, ANYWHERE],
        out_specs=[IN_VMEM, IN_VMEM],
        out_shape=[jax.ShapeDtypeStruct((rows, 2 * LANES), BF16)] * 2,
        scratch_shapes=[
            pltpu.VMEM((steps, rows, depth), BF16),
            pltpu.VMEM((steps, depth, rank), BF16),
            pltpu.VMEM((rows, rank), F32),
            pltpu.SemaphoreType.DMA((2 * steps,)),
        ],
        cost_estimate=pl.CostEstimate(
            flops=2 * rows * width * rank,
            bytes_accessed=2 * width * (rows + rank),
            transcendentals=0,
        ),
        compiler_params=pltpu.CompilerParams(vmem_limit_bytes=PROJECT_VMEM),
        name="project",
    )(activations, projection)


def load(cot_t, half):
    f_local, tokens = cot_t.shape
    f_half = f_local // 2

    def kernel(source, out, sem):
        copy = pltpu.make_async_copy(source.at[pl.ds(half * f_half, f_half), :], out, sem)
        copy.start()
        copy.wait()

    return pl.pallas_call(
        kernel,
        in_specs=[ANYWHERE],
        out_specs=IN_VMEM,
        out_shape=jax.ShapeDtypeStruct((f_half, tokens), BF16),
        scratch_shapes=[pltpu.SemaphoreType.DMA],
        cost_estimate=pl.CostEstimate(
            flops=2 * f_half * tokens, bytes_accessed=4 * f_half * tokens, transcendentals=0
        ),
        compiler_params=pltpu.CompilerParams(vmem_limit_bytes=LOAD_VMEM),
        name="load",
    )(cot_t)


def token_sum(cots, blocks, masks, total, halves):
    f_half = cots[0].shape[0]
    f_local = 2 * f_half
    rows, cols = blocks[0].shape
    n = len(blocks)
    has_total = total is not None
    tile = TOKEN_TILE if f_half % TOKEN_TILE == 0 else f_half

    def kernel(cot_0, cot_1, *refs):
        projected, rest = refs[:n], refs[n:]
        me = lax.axis_index("tensor")
        odd = me % 2
        tokens = [lanes_of(me ^ (even + odd * (uneven - even)), rows) for even, uneven in masks]
        p = jnp.concatenate([ref[...] for ref in projected], axis=0)
        for start in range(0, f_local, tile):
            here, within = pl.ds(start, tile), pl.ds(start % f_half, tile)
            cot = (cot_0, cot_1)[start // f_half]
            c = jnp.concatenate([cot[within, t] for t in tokens], axis=1)
            acc = jnp.dot(c, p, preferred_element_type=F32)
            if has_total:
                acc += rest[0][here, :]
            if halves:
                rest[-2 + start // f_half][within, :] = acc.astype(BF16)
            else:
                rest[-1][here, :] = acc

    if halves:
        out_shape = [jax.ShapeDtypeStruct((f_half, cols), BF16)] * 2
    else:
        out_shape = [jax.ShapeDtypeStruct((f_local, cols), F32)]
    out = pl.pallas_call(
        kernel,
        in_specs=[IN_VMEM] * (2 + n + has_total),
        out_specs=[IN_VMEM] * len(out_shape),
        out_shape=out_shape,
        cost_estimate=pl.CostEstimate(
            flops=2 * n * rows * cols * f_local,
            bytes_accessed=2 * n * rows * (f_local + cols) + 4 * f_local * cols,
            transcendentals=0,
        ),
        compiler_params=pltpu.CompilerParams(vmem_limit_bytes=TOKEN_VMEM),
        name="token_sum",
    )(*cots, *blocks, *([total] if has_total else []))
    return out if halves else out[0]


def pair_sum(kept, met, half):
    f_half = met.shape[0]

    def kernel(kept_ref, met_ref, out):
        mine = kept_ref[half * f_half : (half + 1) * f_half, LANES:]
        out[...] = (mine + met_ref[:, LANES:].astype(F32)).astype(BF16)

    return pl.pallas_call(
        kernel,
        in_specs=[IN_VMEM] * 2,
        out_specs=IN_VMEM,
        out_shape=jax.ShapeDtypeStruct((f_half, LANES), BF16),
        cost_estimate=pl.CostEstimate(
            flops=f_half * LANES, bytes_accessed=8 * f_half * LANES, transcendentals=0
        ),
        compiler_params=pltpu.CompilerParams(vmem_limit_bytes=SMALL_VMEM),
        name="pair_sum",
    )(kept, met)


def gradient_of(kept_ref, met_ref, across_ref, here):
    own = pl.ds(0, LANES)
    return kept_ref[here, own] + met_ref[:, own].astype(F32) + across_ref[...].astype(F32)


def moved(first, second, grad):
    return 0.9 * first + 0.1 * grad, 0.999 * second + 0.001 * grad * grad


def step_half(scales, kept, met, across, first_t, second_t, half):
    f_half = met.shape[0]

    def kernel(scale, kept_ref, met_ref, across_ref, first, second, step_ref):
        here = pl.ds(half * f_half, f_half)
        grad = gradient_of(kept_ref, met_ref, across_ref, here)
        new_first, new_second = moved(first[here, :], second[here, :], grad)
        first_hat = new_first * scale[0]
        second_hat = new_second * scale[1]
        step_ref[...] = (first_hat / (jnp.sqrt(second_hat) + 1e-08)).astype(BF16)

    return pl.pallas_call(
        kernel,
        in_specs=[pl.BlockSpec(memory_space=pltpu.SMEM)] + [IN_VMEM] * 5,
        out_specs=IN_VMEM,
        out_shape=jax.ShapeDtypeStruct((f_half, LANES), BF16),
        cost_estimate=pl.CostEstimate(
            flops=20 * f_half * LANES, bytes_accessed=18 * f_half * LANES, transcendentals=0
        ),
        compiler_params=pltpu.CompilerParams(vmem_limit_bytes=SMALL_VMEM),
        name="step_half",
    )(scales, kept, met, across, first_t, second_t)


def moments(kept, met, across, first_t, second_t):
    f_half = met[0].shape[0]

    def kernel(kept_ref, met_0, met_1, across_0, across_1, first, second, new_first, new_second):
        for half, (met_ref, across_ref) in enumerate(((met_0, across_0), (met_1, across_1))):
            here = pl.ds(half * f_half, f_half)
            grad = gradient_of(kept_ref, met_ref, across_ref, here)
            new_first[here, :], new_second[here, :] = moved(first[here, :], second[here, :], grad)

    return pl.pallas_call(
        kernel,
        in_specs=[IN_VMEM] * 7,
        out_specs=[IN_VMEM] * 2,
        out_shape=[jax.ShapeDtypeStruct(first_t.shape, F32)] * 2,
        cost_estimate=pl.CostEstimate(
            flops=20 * f_half * LANES, bytes_accessed=40 * f_half * LANES, transcendentals=0
        ),
        compiler_params=pltpu.CompilerParams(vmem_limit_bytes=SMALL_VMEM),
        name="moments",
    )(kept, *met, *across, first_t, second_t)


def apply_steps(steps, local_t, f_local, half, out):
    rows = local_t.shape[1]
    f_half = f_local // 2
    tile = tile_of(f_half)
    count = f_half // tile

    def kernel(*refs):
        w_ref = refs[4]
        out_ref, buf, sems = refs[-3:]
        blocks = row_blocks()
        w = jnp.concatenate([w_ref[lanes_of(blocks[j], LANES), :] for j in (2, 3, 0, 1)], axis=0)
        copies = []
        for k in range(count):
            x = jnp.concatenate([ref[k * tile : (k + 1) * tile, :] for ref in refs[:4]], axis=1)
            buf[k] = jnp.dot(x, w, preferred_element_type=F32).astype(BF16)
            to = out_ref.at[pl.ds(half * f_half + k * tile, tile), :]
            copies.append(pltpu.make_async_copy(buf.at[k], to, sems.at[k]))
            copies[-1].start()
        for copy in copies:
            copy.wait()

    return pl.pallas_call(
        kernel,
        in_specs=[IN_VMEM] * 5 + [ANYWHERE] * (out is not None),
        out_specs=ANYWHERE,
        out_shape=jax.ShapeDtypeStruct((f_local, rows), BF16),
        input_output_aliases={} if out is None else {5: 0},
        scratch_shapes=[pltpu.VMEM((count, tile, rows), BF16), pltpu.SemaphoreType.DMA((count,))],
        cost_estimate=pl.CostEstimate(
            flops=8 * f_half * LANES * rows,
            bytes_accessed=2 * f_half * (rows + 4 * LANES) + 8 * rows * LANES,
            transcendentals=0,
        ),
        compiler_params=pltpu.CompilerParams(vmem_limit_bytes=APPLY_VMEM),
        name="apply_steps",
    )(*steps, local_t, *([] if out is None else [out]))


MASKS = ((0, 0), (1, 1), (2, 4), (5, 3), (3, 5), (4, 2), (6, 6), (7, 7))


def stepped(activations, cotangent, projection, first_moment, second_moment, step_count):
    replica = lax.axis_index("dp")
    cot_t = cotangent.T
    f_local = cot_t.shape[0]

    first_t, second_t = first_moment.T, second_moment.T
    t_value = step_count[0].astype(F32)
    scales = 1.0 / (1.0 - jnp.power(np.array([0.9, 0.999], np.float32), t_value))
    out_rows = projection.shape[0] // lax.axis_size("dp")
    local_t = lax.dynamic_slice_in_dim(projection, replica * out_rows, out_rows, 0).T

    first, second = (2, 4), (4, 2)
    sent = project(activations, projection)
    cots = [load(cot_t, h) for h in range(2)]
    sums = []
    for s, own in zip("ab", sent):
        partner = swap(own, "tensor", 1)
        far = swap_by_core(own, first)
        far_partner = swap_by_core(partner, first)
        corner = swap_by_core(far, second)
        other_far = swap(far, "tensor", 1)
        other_far_partner = swap(far_partner, "tensor", 1)
        other_corner = swap(corner, "tensor", 1)
        near = [own, partner, far, other_far]
        total = token_sum(cots, near, MASKS[:4], None, False)
        rest = [far_partner, other_far_partner, corner, other_corner]
        sums.append(token_sum(cots, rest, MASKS[4:], total, s == "a"))
    to_send, kept = sums

    met = [swap(to_send[h], "dp", 1) for h in range(2)]
    across = [swap(pair_sum(kept, met[h], h), "dp", 2) for h in range(2)]
    steps = [step_half(scales, kept, met[h], across[h], first_t, second_t, h) for h in range(2)]
    new_first, new_second = moments(kept, met, across, first_t, second_t)
    update = None
    for h in range(2):
        step_2 = swap(steps[h], "dp", 2)
        step_1 = swap(steps[h], "dp", 1)
        step_3 = swap(step_2, "dp", 1)
        update = apply_steps([steps[h], step_2, step_1, step_3], local_t, f_local, h, update)
    return update.T, new_first.T, new_second.T


def solution(mesh):
    in_specs = (
        P(("dp", "tensor"), None),
        P("dp", "tensor"),
        P(),
        P("dp", "tensor"),
        P("dp", "tensor"),
        P(),
    )
    out_specs = (P("dp", "tensor"), P("dp", "tensor"), P("dp", "tensor"))
    exchanges = mesh.shape["dp"] == 4 and mesh.shape["tensor"] == 8

    def per_device(activations, cotangent, projection, first_moment, second_moment, step_count):
        fits = (
            exchanges
            and first_moment.shape[0] == LANES
            and cotangent.shape[1] % 16 == 0
            and activations.shape[0] % LANES == 0
        )
        if not fits:
            return plain(
                activations, cotangent, projection, first_moment, second_moment, step_count
            )
        return stepped(activations, cotangent, projection, first_moment, second_moment, step_count)

    return jax.shard_map(
        per_device, mesh=mesh, in_specs=in_specs, out_specs=out_specs, check_vma=False
    )
```

```python
import jax
import jax.numpy as jnp
import numpy as np
from jax import lax
from jax.experimental import pallas as pl
from jax.experimental.pallas import tpu as pltpu
from jax.sharding import PartitionSpec as P


F32 = jnp.float32
BF16 = jnp.bfloat16
PROJECT_VMEM = 51 << 20
TOKEN_VMEM = 16 << 20
APPLY_VMEM = 12 << 20
SMALL_VMEM = 4 << 20
LOAD_VMEM = 47 << 20
TOKEN_TILE = 344
LANES = 128


def adam(grad, first_moment, second_moment, step_count):
    t_value = step_count[0].astype(F32)
    new_first = 0.9 * first_moment + 0.1 * grad
    new_second = 0.999 * second_moment + 0.001 * grad * grad
    first_hat = new_first / (1.0 - jnp.power(F32(0.9), t_value))
    second_hat = new_second / (1.0 - jnp.power(F32(0.999), t_value))
    normalized = (first_hat / (jnp.sqrt(second_hat) + 1e-08)).astype(BF16)
    return new_first, new_second, normalized


def plain(activations, cotangent, projection, first_moment, second_moment, step_count):
    projected = jnp.dot(activations, projection, preferred_element_type=F32).astype(BF16)
    partial_grad = lax.dot_general(
        lax.all_gather(projected, "tensor", axis=0, tiled=True),
        cotangent,
        (((0,), (0,)), ((), ())),
        preferred_element_type=F32,
    )
    grad = lax.psum_scatter(partial_grad, "dp", scatter_dimension=0, tiled=True)
    new_first, new_second, normalized = adam(grad, first_moment, second_moment, step_count)
    whole_steps = lax.all_gather(normalized, "dp", axis=0, tiled=True)
    out_rows = projection.shape[0] // lax.axis_size("dp")
    local_projection = lax.dynamic_slice_in_dim(
        projection, lax.axis_index("dp") * out_rows, out_rows, 0
    )
    update = jnp.dot(local_projection, whole_steps, preferred_element_type=F32).astype(BF16)
    return update, new_first, new_second


def tile_of(extent, most=512):
    return max(d for d in range(8, most + 1, 8) if extent % d == 0)


def swap(x, axis, mask):
    return lax.ppermute(x, axis, [(i, i ^ mask) for i in range(lax.axis_size(axis))])


def swap_by_core(x, masks):
    return lax.ppermute(
        x, "tensor", [(i, i ^ masks[i % 2]) for i in range(lax.axis_size("tensor"))]
    )


def row_blocks():
    replica = lax.axis_index("dp")
    return [replica ^ mask for mask in (1, 3, 0, 2)]


def lanes_of(index, size):
    return pl.ds(pl.multiple_of(index * size, size), size)


IN_VMEM = pl.BlockSpec(memory_space=pltpu.VMEM)
ANYWHERE = pl.BlockSpec(memory_space=pl.ANY)


def project(activations, projection):
    rows, width = activations.shape
    rank = projection.shape[1]
    steps = 8
    depth = width // steps

    def kernel(a_hbm, w_hbm, first, second, a_buf, w_buf, acc, sems):
        copies = []
        for k in range(steps):
            part = pl.ds(k * depth, depth)
            a_copy = pltpu.make_async_copy(a_hbm.at[:, part], a_buf.at[k], sems.at[2 * k])
            w_copy = pltpu.make_async_copy(w_hbm.at[part, :], w_buf.at[k], sems.at[2 * k + 1])
            a_copy.start()
            w_copy.start()
            copies.append((a_copy, w_copy))
        total = None
        for k, (a_copy, w_copy) in enumerate(copies):
            a_copy.wait()
            w_copy.wait()
            part = jnp.dot(a_buf[k], w_buf[k], preferred_element_type=F32)
            total = part if total is None else total + part
        acc[...] = total
        for j, block in enumerate(row_blocks()):
            out = (first, second)[j // 2]
            out[:, (j % 2) * LANES : (j % 2 + 1) * LANES] = acc[:, lanes_of(block, LANES)].astype(BF16)

    return pl.pallas_call(
        kernel,
        in_specs=[ANYWHERE, ANYWHERE],
        out_specs=[IN_VMEM, IN_VMEM],
        out_shape=[jax.ShapeDtypeStruct((rows, 2 * LANES), BF16)] * 2,
        scratch_shapes=[
            pltpu.VMEM((steps, rows, depth), BF16),
            pltpu.VMEM((steps, depth, rank), BF16),
            pltpu.VMEM((rows, rank), F32),
            pltpu.SemaphoreType.DMA((2 * steps,)),
        ],
        cost_estimate=pl.CostEstimate(
            flops=2 * rows * width * rank,
            bytes_accessed=2 * width * (rows + rank),
            transcendentals=0,
        ),
        compiler_params=pltpu.CompilerParams(vmem_limit_bytes=PROJECT_VMEM),
        name="project",
    )(activations, projection)


def load(cot_t, half):
    f_local, tokens = cot_t.shape
    f_half = f_local // 2

    def kernel(source, out, sem):
        copy = pltpu.make_async_copy(source.at[pl.ds(half * f_half, f_half), :], out, sem)
        copy.start()
        copy.wait()

    return pl.pallas_call(
        kernel,
        in_specs=[ANYWHERE],
        out_specs=IN_VMEM,
        out_shape=jax.ShapeDtypeStruct((f_half, tokens), BF16),
        scratch_shapes=[pltpu.SemaphoreType.DMA],
        cost_estimate=pl.CostEstimate(
            flops=2 * f_half * tokens, bytes_accessed=4 * f_half * tokens, transcendentals=0
        ),
        compiler_params=pltpu.CompilerParams(vmem_limit_bytes=LOAD_VMEM),
        name="load",
    )(cot_t)


def token_sum(cots, blocks, masks, total, halves, base=0):
    f_half = cots[0].shape[0]
    parts = len(cots)
    f_local = parts * f_half
    rows, cols = blocks[0].shape
    n = len(blocks)
    has_total = total is not None
    tile = TOKEN_TILE if f_half % TOKEN_TILE == 0 else f_half

    def kernel(*refs):
        cot_refs, projected, rest = refs[:parts], refs[parts : parts + n], refs[parts + n :]
        me = lax.axis_index("tensor")
        odd = me % 2
        tokens = [lanes_of(me ^ (even + odd * (uneven - even)), rows) for even, uneven in masks]
        p = jnp.concatenate([ref[...] for ref in projected], axis=0)
        for start in range(0, f_local, tile):
            here, within = pl.ds(start, tile), pl.ds(start % f_half, tile)
            cot = cot_refs[start // f_half]
            c = jnp.concatenate([cot[within, t] for t in tokens], axis=1)
            acc = jnp.dot(c, p, preferred_element_type=F32)
            if has_total:
                acc += rest[0][pl.ds(base + start, tile), :]
            if halves:
                rest[start // f_half - parts][within, :] = acc.astype(BF16)
            else:
                rest[-1][here, :] = acc

    if halves:
        out_shape = [jax.ShapeDtypeStruct((f_half, cols), BF16)] * parts
    else:
        out_shape = [jax.ShapeDtypeStruct((f_local, cols), F32)]
    out = pl.pallas_call(
        kernel,
        in_specs=[IN_VMEM] * (parts + n + has_total),
        out_specs=[IN_VMEM] * len(out_shape),
        out_shape=out_shape,
        cost_estimate=pl.CostEstimate(
            flops=2 * n * rows * cols * f_local,
            bytes_accessed=2 * n * rows * (f_local + cols) + 4 * f_local * cols,
            transcendentals=0,
        ),
        compiler_params=pltpu.CompilerParams(vmem_limit_bytes=TOKEN_VMEM),
        name="token_sum",
    )(*cots, *blocks, *([total] if has_total else []))
    return out if halves else out[0]


def pair_sum(kept, met, half):
    f_half = met.shape[0]

    def kernel(kept_ref, met_ref, out):
        mine = kept_ref[half * f_half : (half + 1) * f_half, LANES:]
        out[...] = (mine + met_ref[:, LANES:].astype(F32)).astype(BF16)

    return pl.pallas_call(
        kernel,
        in_specs=[IN_VMEM] * 2,
        out_specs=IN_VMEM,
        out_shape=jax.ShapeDtypeStruct((f_half, LANES), BF16),
        cost_estimate=pl.CostEstimate(
            flops=f_half * LANES, bytes_accessed=8 * f_half * LANES, transcendentals=0
        ),
        compiler_params=pltpu.CompilerParams(vmem_limit_bytes=SMALL_VMEM),
        name="pair_sum",
    )(kept, met)


def gradient_of(kept_ref, met_ref, across_ref, here):
    own = pl.ds(0, LANES)
    return kept_ref[here, own] + met_ref[:, own].astype(F32) + across_ref[...].astype(F32)


def moved(first, second, grad):
    return 0.9 * first + 0.1 * grad, 0.999 * second + 0.001 * grad * grad


def step_half(scales, kept, met, across, first_t, second_t, half):
    f_half = met.shape[0]

    def kernel(scale, kept_ref, met_ref, across_ref, first, second, step_ref):
        here = pl.ds(half * f_half, f_half)
        grad = gradient_of(kept_ref, met_ref, across_ref, here)
        new_first, new_second = moved(first[here, :], second[here, :], grad)
        first_hat = new_first * scale[0]
        second_hat = new_second * scale[1]
        step_ref[...] = (first_hat / (jnp.sqrt(second_hat) + 1e-08)).astype(BF16)

    return pl.pallas_call(
        kernel,
        in_specs=[pl.BlockSpec(memory_space=pltpu.SMEM)] + [IN_VMEM] * 5,
        out_specs=IN_VMEM,
        out_shape=jax.ShapeDtypeStruct((f_half, LANES), BF16),
        cost_estimate=pl.CostEstimate(
            flops=20 * f_half * LANES, bytes_accessed=18 * f_half * LANES, transcendentals=0
        ),
        compiler_params=pltpu.CompilerParams(vmem_limit_bytes=SMALL_VMEM),
        name="step_half",
    )(scales, kept, met, across, first_t, second_t)


def moments(kept, met, across, first_t, second_t):
    f_half = met[0].shape[0]

    def kernel(kept_ref, met_0, met_1, across_0, across_1, first, second, new_first, new_second):
        for half, (met_ref, across_ref) in enumerate(((met_0, across_0), (met_1, across_1))):
            here = pl.ds(half * f_half, f_half)
            grad = gradient_of(kept_ref, met_ref, across_ref, here)
            new_first[here, :], new_second[here, :] = moved(first[here, :], second[here, :], grad)

    return pl.pallas_call(
        kernel,
        in_specs=[IN_VMEM] * 7,
        out_specs=[IN_VMEM] * 2,
        out_shape=[jax.ShapeDtypeStruct(first_t.shape, F32)] * 2,
        cost_estimate=pl.CostEstimate(
            flops=20 * f_half * LANES, bytes_accessed=40 * f_half * LANES, transcendentals=0
        ),
        compiler_params=pltpu.CompilerParams(vmem_limit_bytes=SMALL_VMEM),
        name="moments",
    )(kept, *met, *across, first_t, second_t)


def apply_steps(steps, local_t, f_local, half, out):
    rows = local_t.shape[1]
    f_half = f_local // 2
    tile = tile_of(f_half)
    count = f_half // tile

    def kernel(*refs):
        w_ref = refs[4]
        out_ref, buf, sems = refs[-3:]
        blocks = row_blocks()
        w = jnp.concatenate([w_ref[lanes_of(blocks[j], LANES), :] for j in (2, 3, 0, 1)], axis=0)
        copies = []
        for k in range(count):
            x = jnp.concatenate([ref[k * tile : (k + 1) * tile, :] for ref in refs[:4]], axis=1)
            buf[k] = jnp.dot(x, w, preferred_element_type=F32).astype(BF16)
            to = out_ref.at[pl.ds(half * f_half + k * tile, tile), :]
            copies.append(pltpu.make_async_copy(buf.at[k], to, sems.at[k]))
            copies[-1].start()
        for copy in copies:
            copy.wait()

    return pl.pallas_call(
        kernel,
        in_specs=[IN_VMEM] * 5 + [ANYWHERE] * (out is not None),
        out_specs=ANYWHERE,
        out_shape=jax.ShapeDtypeStruct((f_local, rows), BF16),
        input_output_aliases={} if out is None else {5: 0},
        scratch_shapes=[pltpu.VMEM((count, tile, rows), BF16), pltpu.SemaphoreType.DMA((count,))],
        cost_estimate=pl.CostEstimate(
            flops=8 * f_half * LANES * rows,
            bytes_accessed=2 * f_half * (rows + 4 * LANES) + 8 * rows * LANES,
            transcendentals=0,
        ),
        compiler_params=pltpu.CompilerParams(vmem_limit_bytes=APPLY_VMEM),
        name="apply_steps",
    )(*steps, local_t, *([] if out is None else [out]))


MASKS = ((0, 0), (1, 1), (2, 4), (5, 3), (3, 5), (4, 2), (6, 6), (7, 7))


def stepped(activations, cotangent, projection, first_moment, second_moment, step_count):
    replica = lax.axis_index("dp")
    cot_t = cotangent.T
    f_local = cot_t.shape[0]

    first_t, second_t = first_moment.T, second_moment.T
    t_value = step_count[0].astype(F32)
    scales = 1.0 / (1.0 - jnp.power(np.array([0.9, 0.999], np.float32), t_value))
    out_rows = projection.shape[0] // lax.axis_size("dp")
    local_t = lax.dynamic_slice_in_dim(projection, replica * out_rows, out_rows, 0).T

    first, second = (2, 4), (4, 2)
    sent = project(activations, projection)
    cots = [load(cot_t, h) for h in range(2)]
    sums = []
    for s, own in zip("ab", sent):
        partner = swap(own, "tensor", 1)
        far = swap_by_core(own, first)
        far_partner = swap_by_core(partner, first)
        corner = swap_by_core(far, second)
        other_far = swap(far, "tensor", 1)
        other_far_partner = swap(far_partner, "tensor", 1)
        other_corner = swap(corner, "tensor", 1)
        near = [own, partner, far, other_far]
        total = token_sum(cots, near, MASKS[:4], None, False)
        rest = [far_partner, other_far_partner, corner, other_corner]
        if s == "a":
            for h in range(2):
                base = h * cots[0].shape[0]
                sums += token_sum([cots[h]], rest, MASKS[4:], total, True, base)
        else:
            sums.append(token_sum(cots, rest, MASKS[4:], total, False))
    *to_send, kept = sums

    met = [swap(to_send[h], "dp", 1) for h in range(2)]
    across = [swap(pair_sum(kept, met[h], h), "dp", 2) for h in range(2)]
    steps = [step_half(scales, kept, met[h], across[h], first_t, second_t, h) for h in range(2)]
    new_first, new_second = moments(kept, met, across, first_t, second_t)
    update = None
    for h in range(2):
        step_2 = swap(steps[h], "dp", 2)
        step_1 = swap(steps[h], "dp", 1)
        step_3 = swap(step_2, "dp", 1)
        update = apply_steps([steps[h], step_2, step_1, step_3], local_t, f_local, h, update)
    return update.T, new_first.T, new_second.T


def solution(mesh):
    in_specs = (
        P(("dp", "tensor"), None),
        P("dp", "tensor"),
        P(),
        P("dp", "tensor"),
        P("dp", "tensor"),
        P(),
    )
    out_specs = (P("dp", "tensor"), P("dp", "tensor"), P("dp", "tensor"))
    exchanges = mesh.shape["dp"] == 4 and mesh.shape["tensor"] == 8

    def per_device(activations, cotangent, projection, first_moment, second_moment, step_count):
        fits = (
            exchanges
            and first_moment.shape[0] == LANES
            and cotangent.shape[1] % 16 == 0
            and activations.shape[0] % LANES == 0
        )
        if not fits:
            return plain(
                activations, cotangent, projection, first_moment, second_moment, step_count
            )
        return stepped(activations, cotangent, projection, first_moment, second_moment, step_count)

    return jax.shard_map(
        per_device, mesh=mesh, in_specs=in_specs, out_specs=out_specs, check_vma=False
    )
```
